32 devices in a mesh: lon: 8 (over y, x, core), lat: 4 (over z).
Axes of the slice: x: 2, y: 2, z: 4, core: 2. Of those that a mesh axis runs over, the one named last changes fastest.
Arguments:
- normed: bfloat16 [8, 96, 192, 192], P(None, 'lat', 'lon'), may hold values from -6 to 6
- cotangent: bfloat16 [8, 96, 192, 192], P(None, 'lat', 'lon'), may hold values from -6 to 6
- weight_qkv: bfloat16 [192, 576], replicated, may hold values from -0.4375 to 0.4375
- weight_proj: bfloat16 [192, 192], replicated, may hold values from -0.4375 to 0.4375
- bias_table: bfloat16 [64, 6, 20736], P('lat'), may hold values from -6 to 390
Outputs:
- input_grad: bfloat16 [8, 96, 192, 192], P(None, 'lat', 'lon')
- qkv_grad: float32 [192, 576], replicated
- proj_grad: float32 [192, 192], replicated
- bias_grad: float32 [64, 6, 20736], P('lat')
The draws below stay inside these ranges and needn't reach their ends.
All inputs are finite; a program needn't handle non-finite values.
Results may differ from the reference program's by a relative error of at most 0.019.
Values may be sent and summed in bfloat16 or wider, within the bound.
No kernel may reach another device: no remote copies, remote signals or barrier semaphores. Data moves between devices by JAX's collectives and lax.ppermute only.
A program may use at most 192 MiB of HBM per device.

```python
import jax
import jax.numpy as jnp
from jax import lax

C = 192
HEADS = 6
WIN_Z = 2
WIN_LAT = 6
WIN_LON = 12
WTOK = 144
NZ = 8
TYPES = 64
NLAT = 96
NLON = 192


def draw_bias_table(key, part):
    keys_list = jax.random.split(jax.random.fold_in(key, 17), 1)
    shape = (TYPES, HEADS, WTOK, WTOK)
    baseline = jnp.clip(jax.random.normal(keys_list[0], shape, jnp.float32), -6.0, 6.0)
    return baseline.reshape(TYPES, HEADS, WTOK * WTOK).astype(jnp.bfloat16)


def block_levels(stream_key, shape, shards, least, largest):
    factor_of, own = 1.0, jax.random.fold_in(stream_key, 6)
    for position, blocks in shards:
        heights = jnp.exp(jax.random.uniform(jax.random.fold_in(own, position), (blocks,), jnp.float32, least / len(shards), largest / len(shards)))
        factor_of = factor_of * jnp.repeat(heights, shape[position] // blocks).reshape([-1 if axis == position else 1 for axis in range(len(shape))])
    return factor_of


def gaussian(rng, dims, width, most, cuts=(), kind=jnp.bfloat16):
    level = block_levels(rng, dims, cuts, -0.22, 0.18) if cuts else 1.0
    entries = jax.random.normal(rng, dims, jnp.float32) * width * level
    return jnp.minimum(jnp.maximum(entries, -most), most).astype(kind)


def setup_inputs(seed: int = 0) -> dict:
    keys = jax.random.split(jax.random.key(seed), 6)
    return {
        "normed": gaussian(keys[0], (NZ, NLAT, NLON, C), 1.0, 6.0, ((1, 4), (2, 8))),
        "cotangent": gaussian(keys[1], (NZ, NLAT, NLON, C), 1.0, 6.0, ((1, 4), (2, 8))),
        "weight_qkv": gaussian(keys[2], (C, 3 * C), C ** -0.5, 0.4375),
        "weight_proj": gaussian(keys[3], (C, C), C ** -0.5, 0.4375),
        "bias_table": draw_bias_table(jax.random.fold_in(keys[5], 71), 0),
    }


def window_split(grid_field):
    levels, height, breadth = grid_field.shape[:3]
    trailing_dims = grid_field.shape[3:]
    shaped = grid_field.reshape((levels // WIN_Z, WIN_Z, height // WIN_LAT, WIN_LAT, breadth // WIN_LON, WIN_LON) + trailing_dims)
    axes_order = (0, 2, 4, 1, 3, 5) + tuple(range(6, 6 + len(trailing_dims)))
    return shaped.transpose(axes_order).reshape((-1, WTOK) + trailing_dims)


def window_merge(windowed, levels, height, breadth):
    channels = windowed.shape[-1]
    shaped = windowed.reshape(levels // WIN_Z, height // WIN_LAT, breadth // WIN_LON, WIN_Z, WIN_LAT, WIN_LON, channels)
    return shaped.transpose(0, 3, 1, 4, 2, 5, 6).reshape(levels, height, breadth, channels)


def window_backward(block_in, block_cot, block_region, block_live, block_types, bias_rows, weight_qkv, weight_proj):
    windows = block_in.shape[0]
    channels = block_in.shape[2]
    head_dim = channels // HEADS
    softmax_scale = head_dim ** -0.5
    high = lax.Precision.HIGHEST
    f32 = jnp.float32
    projected = jnp.einsum('bnc,cf->bnf', block_in.astype(f32), weight_qkv.astype(f32), precision=high).astype(jnp.bfloat16)
    projected = projected.reshape(windows, WTOK, 3, HEADS, head_dim)
    queries = projected[:, :, 0]
    key_rows = projected[:, :, 1]
    values = projected[:, :, 2]
    bias_add = jnp.dot(block_types, bias_rows.astype(f32), precision=high).reshape(windows, HEADS, WTOK, WTOK)
    scores = jnp.einsum('bqhd,bkhd->bhqk', queries.astype(f32), key_rows.astype(f32), precision=high) * softmax_scale + bias_add
    allowed = (block_region[:, :, None] == block_region[:, None, :]) & (block_live[:, :, None] == block_live[:, None, :])
    allowed = allowed[:, None]
    peak_score = jnp.max(jnp.where(allowed, scores, -1e30), axis=-1, keepdims=True)
    exp_terms = jnp.where(allowed, jnp.exp(scores - peak_score), 0.0)
    attn_probs = exp_terms / jnp.sum(exp_terms, axis=-1, keepdims=True)
    probs_b = attn_probs.astype(jnp.bfloat16)
    mixed = jnp.einsum('bhqk,bkhd->bqhd', probs_b.astype(f32), values.astype(f32), precision=high).astype(jnp.bfloat16)
    mixed = mixed.reshape(windows, WTOK, channels)
    grad_proj = jnp.einsum('bnc,bnf->cf', mixed.astype(f32), block_cot.astype(f32), precision=high)
    mixed_grad = jnp.einsum('bnf,cf->bnc', block_cot.astype(f32), weight_proj.astype(f32), precision=high).astype(jnp.bfloat16)
    mixed_grad = mixed_grad.reshape(windows, WTOK, HEADS, head_dim)
    prob_grad = jnp.einsum('bqhd,bkhd->bhqk', mixed_grad.astype(f32), values.astype(f32), precision=high)
    row_delta = jnp.sum(attn_probs * prob_grad, axis=-1, keepdims=True)
    score_grad = attn_probs * (prob_grad - row_delta)
    grad_bias = jnp.dot(block_types.T, score_grad.reshape(windows, -1), precision=high)
    score_grad_b = score_grad.astype(jnp.bfloat16).astype(f32)
    query_grad = (jnp.einsum('bhqk,bkhd->bqhd', score_grad_b, key_rows.astype(f32), precision=high) * softmax_scale).astype(jnp.bfloat16)
    key_grad = (jnp.einsum('bhqk,bqhd->bkhd', score_grad_b, queries.astype(f32), precision=high) * softmax_scale).astype(jnp.bfloat16)
    value_grad = jnp.einsum('bhqk,bqhd->bkhd', probs_b.astype(f32), mixed_grad.astype(f32), precision=high).astype(jnp.bfloat16)
    cols_grad = jnp.stack([query_grad, key_grad, value_grad], axis=2).reshape(windows, WTOK, 3 * channels)
    grad_qkv = jnp.einsum('bnc,bnf->cf', block_in.astype(f32), cols_grad.astype(f32), precision=high)
    grad_in = jnp.einsum('bnf,cf->bnc', cols_grad.astype(f32), weight_qkv.astype(f32), precision=high).astype(jnp.bfloat16)
    return grad_in, grad_qkv, grad_proj, grad_bias


def reference(normed, cotangent, weight_qkv, weight_proj, bias_table):
    levels, height, breadth, channels = normed.shape
    level_shift = WIN_Z // 2
    lat_shift = WIN_LAT // 2
    lon_shift = WIN_LON // 2

    def to_frame(grid_field):
        rolled = jnp.roll(jnp.roll(grid_field, -lon_shift, axis=2), -level_shift, axis=0)
        padding = jnp.zeros((levels, lat_shift, breadth, channels), grid_field.dtype)
        return jnp.concatenate([rolled[:, lat_shift:], padding], axis=1)

    framed_in = window_split(to_frame(normed))
    framed_cot = window_split(to_frame(cotangent))
    level_index = jnp.arange(levels, dtype=jnp.int32)
    wrapped_levels = (level_index >= levels - level_shift).astype(jnp.int32)
    wrapped_field = jnp.broadcast_to(wrapped_levels[:, None, None], (levels, height, breadth))
    region_win = window_split(wrapped_field)
    row_index = jnp.arange(height, dtype=jnp.int32)
    live_rows = row_index < height - lat_shift
    live_field = jnp.broadcast_to(live_rows[None, :, None], (levels, height, breadth))
    live_win = window_split(live_field)
    level_windows = levels // WIN_Z
    lat_windows = height // WIN_LAT
    lon_windows = breadth // WIN_LON
    level_part = jnp.arange(level_windows, dtype=jnp.int32)[:, None, None]
    lat_part = jnp.arange(lat_windows, dtype=jnp.int32)[None, :, None]
    kinds = jnp.broadcast_to(lat_part * level_windows + level_part, (level_windows, lat_windows, lon_windows))
    onehot = (kinds.reshape(-1)[:, None] == jnp.arange(TYPES, dtype=jnp.int32)[None, :]).astype(jnp.float32)
    bias_rows = bias_table.reshape(TYPES, -1)
    window_total = framed_in.shape[0]
    block_size = max(divisor for divisor in range(1, 65) if window_total % divisor == 0)
    blocks = window_total // block_size

    def regroup(array):
        return array.reshape((blocks, block_size) + array.shape[1:])

    def step_block(totals, pieces):
        grad_in, grad_qkv, grad_proj, grad_bias = window_backward(pieces[0], pieces[1], pieces[2], pieces[3], pieces[4], bias_rows, weight_qkv, weight_proj)
        return (totals[0] + grad_qkv, totals[1] + grad_proj, totals[2] + grad_bias), grad_in

    start = (jnp.zeros((channels, 3 * channels), jnp.float32), jnp.zeros((channels, channels), jnp.float32), jnp.zeros((TYPES, HEADS * WTOK * WTOK), jnp.float32))
    totals, grads = lax.scan(step_block, start, (regroup(framed_in), regroup(framed_cot), regroup(region_win), regroup(live_win), regroup(onehot)))
    framed_grad = window_merge(grads.reshape(window_total, WTOK, channels), levels, height, breadth)
    zeros_rows = jnp.zeros((levels, lat_shift, breadth, channels), jnp.bfloat16)
    unshifted = jnp.concatenate([zeros_rows, framed_grad[:, :height - lat_shift]], axis=1)
    input_grad = jnp.roll(jnp.roll(unshifted, lon_shift, axis=2), level_shift, axis=0)
    return input_grad, totals[0], totals[1], totals[2].reshape(TYPES, HEADS, WTOK * WTOK)
```

```python
import math

import jax
import jax.numpy as jnp
from jax import lax
from jax.experimental import pallas as pl
from jax.experimental.pallas import tpu as pltpu
from jax.sharding import PartitionSpec as P

HEADS = 6
WIN_Z = 2
WIN_LAT = 6
WIN_LON = 12
WTOK = 144
ROWS_PER_GROUP = 8
GROUP = ROWS_PER_GROUP * WTOK
LOG2E = math.log2(math.e)
NT = (((1,), (1,)), ((), ()))
TN = (((0,), (0,)), ((), ()))
NN = (((1,), (0,)), ((), ()))
F32 = jnp.float32
BF16 = jnp.bfloat16


def mm(lhs, rhs, dims=NN):
    return lax.dot_general(lhs, rhs, dims, preferred_element_type=F32)


def from_behind(block, axis, distance):
    devices = range(lax.axis_size(axis))
    route = [((i - distance) % len(devices), i) for i in devices]
    return lax.ppermute(block, axis, route)


def passed_along(block, axis, distance):
    devices = range(lax.axis_size(axis))
    route = [(i - distance, i) for i in devices if i - distance in devices]
    return lax.ppermute(block, axis, route)


def kind_kernel(
    flag_ref, x0_ref, x1_ref, c0_ref, c1_ref, wq_ref, wk_ref, wv_ref, wp_ref, bias_ref,
    gx_ref, gq_ref, gk_ref, gv_ref, gp_ref, gb_ref,
    bias_rows, grad_rows,
):
    lat_step = pl.program_id(0)
    level_step = pl.program_id(1)
    first = (lat_step == 0) & (level_step == 0)
    rows = x0_ref.shape[1]
    channels = x0_ref.shape[2]
    head_dim = channels // HEADS
    breadth = rows // WIN_LAT
    tokens = WIN_Z * rows
    windows = tokens // WTOK
    scale = head_dim ** (-0.5)

    @pl.when(first)
    def _():
        gq_ref[...] = jnp.zeros_like(gq_ref)
        gk_ref[...] = jnp.zeros_like(gk_ref)
        gv_ref[...] = jnp.zeros_like(gv_ref)
        gp_ref[...] = jnp.zeros_like(gp_ref)

    def bias_group(group, carry):
        piece = bias_ref[0, :, pl.ds(pl.multiple_of(group * GROUP, GROUP), GROUP)].astype(F32) * LOG2E
        for j in range(ROWS_PER_GROUP):
            bias_rows[group * ROWS_PER_GROUP + j, 0:HEADS, 0:WTOK] = piece[:, j * WTOK : (j + 1) * WTOK]
        return carry

    lax.fori_loop(0, WTOK // ROWS_PER_GROUP, bias_group, 0)

    wrapped = level_step == pl.num_programs(1) - 1
    edge = (flag_ref[0] == 1) & (lat_step == pl.num_programs(0) - 1)
    tq = lax.broadcasted_iota(jnp.int32, (WTOK, WTOK), 0)
    tk = lax.broadcasted_iota(jnp.int32, (WTOK, WTOK), 1)
    half = WTOK // WIN_Z
    lat_half = half // 2
    zq = (tq >= half).astype(jnp.int32)
    zk = (tk >= half).astype(jnp.int32)
    yq = (tq - zq * half >= lat_half).astype(jnp.int32)
    yk = (tk - zk * half >= lat_half).astype(jnp.int32)
    bad = (zq ^ zk) * wrapped.astype(jnp.int32) + (yq ^ yk) * edge.astype(jnp.int32)
    mask = jnp.where(bad > 0, -1e30, 0.0)

    out_pos = lax.broadcasted_iota(jnp.int32, (tokens, tokens), 0)
    in_pos = lax.broadcasted_iota(jnp.int32, (tokens, tokens), 1)
    win = out_pos // WTOK
    inside = out_pos - win * WTOK
    line = inside // WIN_LON
    source = line * breadth + win * WIN_LON + (inside - line * WIN_LON)
    perm = (source == in_pos).astype(F32).astype(BF16)

    x_tok = jnp.concatenate([x0_ref[0], x1_ref[0]], axis=0)
    c_tok = jnp.concatenate([c0_ref[0], c1_ref[0]], axis=0)
    x = mm(perm, x_tok).astype(BF16)
    c = mm(perm, c_tok).astype(BF16)
    wq = wq_ref[...]
    wk = wk_ref[...]
    wv = wv_ref[...]
    q_f = mm(x, wq) * (scale * LOG2E)
    q_all = q_f.astype(BF16)
    k_all = mm(x, wk).astype(BF16)
    v_all = mm(x, wv).astype(BF16)
    mg_f = mm(c, wp_ref[...], NT)
    mg_all = mg_f.astype(BF16)

    lane = lax.broadcasted_iota(jnp.int32, (WTOK, channels), 1)
    in_head = [(lane >= h * head_dim) & (lane < (h + 1) * head_dim) for h in range(HEADS)]

    def stacked(part):
        zero = jnp.zeros_like(part)
        return jnp.concatenate([jnp.where(in_head[h], part, zero) for h in range(HEADS)], axis=0)

    mixed = []
    dq = []
    dk = []
    dv = []
    for w in range(windows):
        span = slice(w * WTOK, (w + 1) * WTOK)
        qw = q_all[span]
        kw = k_all[span]
        vw = v_all[span]
        mgw = mg_all[span]
        q_t = q_f[span].T.astype(BF16)
        mg_t = mg_f[span].T.astype(BF16)
        scores = mm(stacked(qw), kw, NT)
        prob_grads = mm(stacked(mgw), vw, NT)
        o_sum = jnp.zeros((WTOK, channels), F32)
        dq_sum = jnp.zeros((WTOK, channels), F32)
        dk_rows = []
        dv_rows = []
        for h in range(HEADS):
            hs = slice(h * WTOK, (h + 1) * WTOK)
            cs = slice(h * head_dim, (h + 1) * head_dim)
            t = scores[hs] + (bias_rows[:, h, :][:, :WTOK] + mask)
            e = jnp.exp2(t - jnp.max(t, axis=1, keepdims=True))
            p = e * (1.0 / jnp.sum(e, axis=1, keepdims=True))
            pb = p.astype(BF16)
            pdp = p * prob_grads[hs]
            ds = pdp - p * jnp.sum(pdp, axis=1, keepdims=True)
            dsb = ds.astype(BF16)
            if w == 0:
                grad_rows[:, h, 0:WTOK] = ds
            else:
                grad_rows[:, h, 0:WTOK] = grad_rows[:, h, 0:WTOK] + ds
            o_sum = jnp.where(in_head[h], mm(pb, vw), o_sum)
            dq_sum = jnp.where(in_head[h], mm(dsb, kw), dq_sum)
            dv_rows.append(mm(mg_t[cs], pb))
            dk_rows.append(mm(q_t[cs], dsb))
        mixed.append(o_sum)
        dq.append(dq_sum * scale)
        dk.append(jnp.concatenate(dk_rows, axis=0).T * (1.0 / LOG2E))
        dv.append(jnp.concatenate(dv_rows, axis=0).T)
    mixed = jnp.concatenate(mixed, axis=0).astype(BF16)
    dq = jnp.concatenate(dq, axis=0).astype(BF16)
    dk = jnp.concatenate(dk, axis=0).astype(BF16)
    dv = jnp.concatenate(dv, axis=0).astype(BF16)
    gp_ref[...] += mm(mixed, c, TN)
    gq_ref[...] += mm(x, dq, TN)
    gk_ref[...] += mm(x, dk, TN)
    gv_ref[...] += mm(x, dv, TN)
    gx = (mm(dq, wq, NT) + mm(dk, wk, NT) + mm(dv, wv, NT)).astype(BF16)
    gx = mm(perm, gx, TN).astype(BF16)
    for z in range(WIN_Z):
        gx_ref[z] = gx[z * rows : (z + 1) * rows]

    def grad_group(group, carry):
        pieces = [
            grad_rows[group * ROWS_PER_GROUP + j, 0:HEADS, 0:WTOK] for j in range(ROWS_PER_GROUP)
        ]
        joined = jnp.concatenate(pieces, axis=1).astype(BF16)
        gb_ref[0, :, pl.ds(pl.multiple_of(group * GROUP, GROUP), GROUP)] = joined
        return carry

    lax.fori_loop(0, WTOK // ROWS_PER_GROUP, grad_group, 0)


def kinds_backward(flag, frame_in, frame_cot, weights, weight_proj, bias_table, lat_range):
    levels, cells, channels = frame_in.shape
    types, heads, pairs = bias_table.shape
    level_windows = levels // WIN_Z
    lat_windows = types // level_windows
    first, last = lat_range
    rows = cells // lat_windows
    count = last - first

    def level_block(offset):
        return pl.BlockSpec(
            (1, rows, channels),
            lambda b, a, *_: ((WIN_Z * a + offset) % levels, b + first, 0),
        )

    def whole(shape):
        return pl.BlockSpec(shape, lambda b, a, *_: (0, 0))

    square = whole((channels, channels))
    x_specs = [level_block(1), level_block(2)]
    f32_square = jax.ShapeDtypeStruct((channels, channels), F32)
    return pl.pallas_call(
        kind_kernel,
        grid_spec=pltpu.PrefetchScalarGridSpec(
            num_scalar_prefetch=1,
            grid=(count, level_windows),
            in_specs=x_specs + x_specs + [square] * 4
            + [
                pl.BlockSpec(
                    (1, heads, pairs), lambda b, a, *_: ((b + first) * level_windows + a, 0, 0)
                )
            ],
            out_specs=[
                pl.BlockSpec((WIN_Z, rows, channels), lambda b, a, *_: (a, b, 0)),
                square, square, square, square,
                pl.BlockSpec((1, heads, pairs), lambda b, a, *_: (b * level_windows + a, 0, 0)),
            ],
            scratch_shapes=[
                pltpu.VMEM((WTOK, 8, 256), F32),
                pltpu.VMEM((WTOK, 8, 256), F32),
            ],
        ),
        out_shape=[
            jax.ShapeDtypeStruct((levels, count * rows, channels), BF16),
            f32_square, f32_square, f32_square, f32_square,
            jax.ShapeDtypeStruct((count * level_windows, heads, pairs), BF16),
        ],
        compiler_params=pltpu.CompilerParams(
            dimension_semantics=("arbitrary", "arbitrary"), vmem_limit_bytes=56 * 1024 * 1024
        ),
    )(flag, frame_in, frame_in, frame_cot, frame_cot, *weights, weight_proj, bias_table)


def local(normed, cotangent, weight_qkv, weight_proj, bias_table):
    levels, height, breadth, channels = normed.shape
    level_shift = WIN_Z // 2
    lat_shift = WIN_LAT // 2
    lon_shift = WIN_LON // 2
    across = from_behind((normed[:, :, :lon_shift], cotangent[:, :, :lon_shift]), "lon", -1)
    wide_in = jnp.concatenate([normed[:, :, lon_shift:], across[0]], axis=2)
    wide_cot = jnp.concatenate([cotangent[:, :, lon_shift:], across[1]], axis=2)
    upward = passed_along((wide_in[:, :lat_shift], wide_cot[:, :lat_shift]), "lat", -1)
    frame_in = jnp.concatenate([wide_in[:, lat_shift:], upward[0]], axis=1)
    frame_cot = jnp.concatenate([wide_cot[:, lat_shift:], upward[1]], axis=1)
    flag = (lax.axis_index("lat") == lax.axis_size("lat") - 1).astype(jnp.int32).reshape(1)
    lat_windows = height // WIN_LAT
    weights = tuple(weight_qkv[:, i * channels : (i + 1) * channels] for i in range(3))
    frame_in = frame_in.reshape(levels, height * breadth, channels)
    frame_cot = frame_cot.reshape(levels, height * breadth, channels)
    framed_grad, gq, gk, gv, gp, gb = kinds_backward(
        flag, frame_in, frame_cot, weights, weight_proj, bias_table, (0, lat_windows)
    )
    framed_grad = framed_grad.reshape(levels, height, breadth, channels)
    returned = passed_along(framed_grad[:, height - lat_shift :], "lat", 1)
    wide_grad = jnp.concatenate([returned, framed_grad[:, : height - lat_shift]], axis=1)
    sideways = from_behind(wide_grad[:, :, breadth - lon_shift :], "lon", 1)
    shifted_grad = jnp.concatenate([sideways, wide_grad[:, :, : breadth - lon_shift]], axis=2)
    input_grad = jnp.roll(shifted_grad, level_shift, axis=0)
    small = jnp.concatenate([gq, gk, gv, gp], axis=1).astype(BF16)
    small = lax.psum(small, ("lat", "lon")).astype(F32)
    bias_grad = lax.psum(gb, "lon").astype(F32)
    return (input_grad, small[:, : 3 * channels], small[:, 3 * channels :], bias_grad)


def solution(mesh):
    in_specs = (
        P(None, "lat", "lon", None),
        P(None, "lat", "lon", None),
        P(),
        P(),
        P("lat", None, None),
    )
    out_specs = (P(None, "lat", "lon", None), P(), P(), P("lat", None, None))
    return jax.shard_map(local, mesh=mesh, in_specs=in_specs, out_specs=out_specs, check_vma=False)
```
